32 devices in a mesh: dp: 8 (over y, x, core), mp: 4 (over z).
Axes of the slice: x: 2, y: 2, z: 4, core: 2. Of those that a mesh axis runs over, the one named last changes fastest.
Arguments:
- hidden_in: bfloat16 [2, 32, 4096], P(None, 'dp', 'mp'), may hold values from -6 to 6
- rec_gain: float32 [2, 4096], replicated, may hold values from 0.5 to 1.5
- rec_in_x: bfloat16 [2, 4096, 4096], P(None, 'dp', 'mp'), may hold values from -0.09375 to 0.09375
- rec_in_y: bfloat16 [2, 4096, 4096], P(None, 'dp', 'mp'), may hold values from -0.09375 to 0.09375
- conv_weight: float32 [2, 4, 4096], P(None, None, 'mp'), may hold values from -3 to 3
- conv_bias: float32 [2, 4096], P(None, 'mp'), may hold values from -3 to 3
- gate_x_weight: bfloat16 [2, 16, 256, 256], P(None, 'mp'), may hold values from -0.375 to 0.375
- gate_x_bias: float32 [2, 4096], P(None, 'mp'), may hold values from -4 to 4
- gate_a_weight: bfloat16 [2, 16, 256, 256], P(None, 'mp'), may hold values from -0.375 to 0.375
- gate_a_bias: float32 [2, 4096], P(None, 'mp'), may hold values from -4 to 4
- decay_param: float32 [2, 4096], P(None, 'mp'), may hold values from -9 to -1
- rec_out: bfloat16 [2, 4096, 4096], P(None, 'dp', 'mp'), may hold values from -0.09375 to 0.09375
- lru_state: bfloat16 [2, 32, 4096], P(None, 'dp', 'mp'), may hold values from -6 to 6
- conv_state: bfloat16 [2, 3, 32, 4096], P(None, None, 'dp', 'mp'), may hold values from -6 to 6
- scale_index: int32 [2], replicated, may hold values from 0 to 7
- attn_gain: float32 [4096], replicated, may hold values from 0.5 to 1.5
- attn_q: bfloat16 [4096, 4096], P('dp', 'mp'), may hold values from -0.09375 to 0.09375
- attn_kv: bfloat16 [4096, 512], P('dp', 'mp'), may hold values from -0.09375 to 0.09375
- attn_out: bfloat16 [4096, 4096], P('dp', 'mp'), may hold values from -0.09375 to 0.09375
- key_cache: bfloat16 [32, 2048, 256], P('dp', 'mp'), may hold values from -400 to 400
- value_cache: bfloat16 [32, 2048, 256], P('dp', 'mp'), may hold values from -6 to 6
- positions: int32 [32], P('dp'), may hold values from 1 to 6143
Outputs:
- hidden_out: bfloat16 [2, 32, 4096], P(None, 'dp', 'mp')
- lru_out: bfloat16 [2, 32, 4096], P(None, 'dp', 'mp')
- conv_out: bfloat16 [2, 3, 32, 4096], P(None, None, 'dp', 'mp')
- new_kv: bfloat16 [2, 32, 512], P(None, 'dp', 'mp')
The draws below stay inside these ranges and needn't reach their ends.
Inputs may be any that keep to these rules, and one draw needn't show every extreme that they name: `positions`: the count of tokens a sequence has seen; the cache holds its last min(that count, 2048) tokens.
All inputs are finite; a program needn't handle non-finite values.
Results may differ from the reference program's by a relative error of at most 0.03.
Values may be sent and summed in bfloat16 or wider, within the bound.
A program may use at most 64 MiB of HBM per device.

```python
import jax
import jax.numpy as jnp
from jax import lax

D = 4096
LRU = 4096
HEADS = 16
HEAD_DIM = 256
WIN = 2048
CONV = 4
LAYERS = 2
STEPS = 2
BATCH = 32


def draw_key_cache(key, part):
    base = jax.random.normal(jax.random.fold_in(key, 11), (BATCH, WIN, HEAD_DIM), jnp.float32)
    return jnp.clip(base, -400.0, 400.0).astype(jnp.bfloat16)


def plant(entries, key, least, high):
    longest = entries.shape.index(max(entries.shape))
    spots = []
    for shift in (0, 1):
        where = [jax.random.randint(jax.random.fold_in(key, axis), (), 0, length) for axis, length in enumerate(entries.shape)]
        where[longest] = (where[longest] + shift) % entries.shape[longest]
        spots.append(tuple(where))
    return entries.at[spots[0]].set(least).at[spots[1]].set(high)


def shard_levels(own_key, shape, cuts, low, high):
    def one(axis_at, shards_of):
        draws = jax.random.uniform(jax.random.fold_in(jax.random.fold_in(own_key, 6), axis_at), (shards_of,), jnp.float32, low / len(cuts), high / len(cuts))
        return jnp.repeat(jnp.exp(draws), shape[axis_at] // shards_of).reshape((-1,) + (1,) * (len(shape) - axis_at - 1))

    factor_of = one(*cuts[0])
    for cut in cuts[1:]:
        factor_of = factor_of * one(*cut)
    return factor_of


def noise(stream_key, shape, width, bound, pieces=(), held_as=jnp.bfloat16):
    array = jax.random.normal(stream_key, shape, jnp.float32) * width
    if len(pieces) > 0:
        array = shard_levels(stream_key, shape, pieces, -0.22, 0.18) * array
    return jnp.clip(array, min=-bound, max=bound).astype(held_as)


def setup_inputs(seed: int = 0) -> dict:
    key_list = jax.random.split(jax.random.key(seed), 23)
    return {
        "hidden_in": noise(key_list[0], (STEPS, BATCH, D), 1.0, 6.0, ((1, 8), (2, 4))),
        "rec_gain": jnp.clip(1.0 + 0.1 * jax.random.normal(key_list[1], (LAYERS, D), jnp.float32), 0.5, 1.5),
        "rec_in_x": noise(key_list[2], (LAYERS, D, LRU), D ** -0.5, 0.09375, ((1, 8), (2, 4))),
        "rec_in_y": noise(key_list[3], (LAYERS, D, LRU), D ** -0.5, 0.09375, ((1, 8), (2, 4))),
        "conv_weight": noise(key_list[4], (LAYERS, CONV, LRU), 0.5, 3.0, ((2, 4),), jnp.float32),
        "conv_bias": noise(key_list[5], (LAYERS, LRU), 0.5, 3.0, ((1, 4),), jnp.float32),
        "gate_x_weight": noise(key_list[6], (LAYERS, HEADS, LRU // HEADS, LRU // HEADS), (LRU // HEADS) ** -0.5, 0.375, ((1, 4),)),
        "gate_x_bias": noise(key_list[7], (LAYERS, LRU), 1.0, 4.0, ((1, 4),), jnp.float32),
        "gate_a_weight": noise(key_list[8], (LAYERS, HEADS, LRU // HEADS, LRU // HEADS), (LRU // HEADS) ** -0.5, 0.375, ((1, 4),)),
        "gate_a_bias": noise(key_list[9], (LAYERS, LRU), 1.0, 4.0, ((1, 4),), jnp.float32),
        "decay_param": jnp.clip(-9.0 + 8.0 * jax.random.uniform(key_list[10], (LAYERS, LRU), jnp.float32) ** shard_levels(key_list[10], (LAYERS, LRU), ((1, 4),), -0.2, 0.2), -9.0, -1.0),
        "rec_out": noise(key_list[11], (LAYERS, LRU, D), LRU ** -0.5, 0.09375, ((1, 8), (2, 4))),
        "lru_state": noise(key_list[12], (LAYERS, BATCH, LRU), 1.0, 6.0, ((1, 8), (2, 4))),
        "conv_state": noise(key_list[13], (LAYERS, CONV - 1, BATCH, LRU), 1.0, 6.0, ((2, 8), (3, 4))),
        "scale_index": jax.random.randint(key_list[14], (LAYERS,), 0, 8).astype(jnp.int32),
        "attn_gain": jnp.clip(1.0 + 0.1 * jax.random.normal(key_list[15], (D,), jnp.float32), 0.5, 1.5),
        "attn_q": noise(key_list[16], (D, HEADS * HEAD_DIM), D ** -0.5, 0.09375, ((0, 8), (1, 4))),
        "attn_kv": noise(key_list[17], (D, 2 * HEAD_DIM), D ** -0.5, 0.09375, ((0, 8), (1, 4))),
        "attn_out": noise(key_list[18], (HEADS * HEAD_DIM, D), (HEADS * HEAD_DIM) ** -0.5, 0.09375, ((0, 8), (1, 4))),
        "key_cache": draw_key_cache(jax.random.fold_in(key_list[22], 71), 0),
        "value_cache": noise(key_list[20], (BATCH, WIN, HEAD_DIM), 1.0, 6.0, ((0, 8), (1, 4))),
        "positions": plant(jax.random.randint(key_list[21], (BATCH,), 1, 3 * WIN), jax.random.fold_in(key_list[21], 1), 1, (3 * WIN) - 1).astype(jnp.int32),
    }


def norm_rows(values, gain):
    mean_sq = lax.optimization_barrier(jnp.mean(values * values, axis=-1, keepdims=True))
    return (values * lax.rsqrt(mean_sq + 1e-06) * gain.astype(jnp.float32)).astype(jnp.bfloat16)

def lru_gate(filtered_half, weight, bias):
    rows = filtered_half.shape[0]
    shaped = filtered_half.reshape(rows, HEADS, LRU // HEADS).astype(jnp.float32)
    mixed = jnp.einsum('bhi,hij->bhj', shaped, weight.astype(jnp.float32))
    return jax.nn.sigmoid(mixed.reshape(rows, LRU) + bias)

def attend(query, key_cache, value_cache, fresh_keys, fresh_values, positions, step):
    rows = query.shape[0]
    heads = query.reshape(rows, HEADS, HEAD_DIM)

    def single(item):
        head_rows, key_rows, value_rows, new_keys, new_values, position = item
        keys = jnp.concatenate([key_rows, new_keys], 0)
        values = jnp.concatenate([value_rows, new_values], 0)
        scores = jnp.dot(head_rows, keys.T, preferred_element_type=jnp.float32) * HEAD_DIM ** (-0.5)
        slot_ids = jnp.arange(WIN, dtype=jnp.int32)
        held = position - 1 - jnp.mod(position - 1 - slot_ids, WIN)
        cached = (held >= 0) & (held >= position + step - WIN + 1)
        valid = jnp.concatenate([cached, jnp.ones((new_keys.shape[0],), dtype=bool)])
        masked = jnp.where(valid[None, :], scores, -1e+30)
        best = lax.optimization_barrier(jnp.max(masked, axis=-1, keepdims=True))
        weights = jnp.where(valid[None, :], jnp.exp(masked - best), 0.0)
        total = lax.optimization_barrier(jnp.sum(weights, axis=-1, keepdims=True))
        summed = jnp.dot(weights.astype(jnp.bfloat16), values, preferred_element_type=jnp.float32)
        return (summed / total).astype(jnp.bfloat16).reshape(HEADS * HEAD_DIM)
    return lax.map(single, (heads, key_cache, value_cache, fresh_keys, fresh_values, positions))

def reference(hidden_in, rec_gain, rec_in_x, rec_in_y, conv_weight, conv_bias, gate_x_weight, gate_x_bias, gate_a_weight, gate_a_bias, decay_param, rec_out, lru_state, conv_state, scale_index, attn_gain, attn_q, attn_kv, attn_out, key_cache, value_cache, positions):
    scales = 2.0 ** ((scale_index.astype(jnp.float32) - 4.0) * 0.5)
    states = [lru_state[layer].astype(jnp.float32) * scales[layer] for layer in range(LAYERS)]
    windows = [conv_state[layer] for layer in range(LAYERS)]
    fresh_keys = []
    fresh_values = []
    outputs = []
    kv_rows = []
    for step in range(STEPS):
        stream = hidden_in[step].astype(jnp.float32)
        for layer in range(LAYERS):
            normed = norm_rows(stream, rec_gain[layer])
            driven = jnp.dot(normed, rec_in_x[layer], preferred_element_type=jnp.float32).astype(jnp.bfloat16)
            gating = jax.nn.gelu(jnp.dot(normed, rec_in_y[layer], preferred_element_type=jnp.float32), approximate=True)
            taps = jnp.concatenate([windows[layer], driven[None]], 0)
            filtered = lax.optimization_barrier(jnp.sum(taps.astype(jnp.float32) * conv_weight[layer][:, None, :], axis=0)) + conv_bias[layer]
            filtered_half = filtered.astype(jnp.bfloat16)
            input_gate = lru_gate(filtered_half, gate_x_weight[layer], gate_x_bias[layer])
            decay_gate = lru_gate(filtered_half, gate_a_weight[layer], gate_a_bias[layer])
            log_decay = -8.0 * decay_gate * jax.nn.softplus(decay_param[layer])
            states[layer] = jnp.exp(log_decay) * states[layer] + jnp.sqrt(1.0 - jnp.exp(2.0 * log_decay)) * (input_gate * filtered)
            mixed = (states[layer] * gating).astype(jnp.bfloat16)
            stream = stream + jnp.dot(mixed, rec_out[layer], preferred_element_type=jnp.float32)
            windows[layer] = taps[1:]
        normed = norm_rows(stream, attn_gain)
        query = jnp.dot(normed, attn_q, preferred_element_type=jnp.float32).astype(jnp.bfloat16)
        key_value = jnp.dot(normed, attn_kv, preferred_element_type=jnp.float32).astype(jnp.bfloat16)
        kv_rows.append(key_value)
        fresh_keys.append(key_value[:, :HEAD_DIM])
        fresh_values.append(key_value[:, HEAD_DIM:])
        attended = attend(query, key_cache, value_cache, jnp.stack(fresh_keys, 1), jnp.stack(fresh_values, 1), positions, step)
        stream = stream + jnp.dot(attended, attn_out, preferred_element_type=jnp.float32)
        outputs.append(stream.astype(jnp.bfloat16))
    lru_new = jnp.stack([(states[layer] / scales[layer]).astype(jnp.bfloat16) for layer in range(LAYERS)], 0)
    return (jnp.stack(outputs, 0), lru_new, jnp.stack(windows, 0), jnp.stack(kv_rows, 0))
```

```python
import functools

import jax
import jax.numpy as jnp
from jax import lax
from jax.experimental import pallas as pl
from jax.experimental.pallas import tpu as pltpu
from jax.sharding import PartitionSpec as P

MESH = pl.DeviceIdType.MESH
LANES = 128
F32 = jnp.float32
BF16 = jnp.bfloat16


def softplus(v):
    return jnp.maximum(v, 0.0) + jnp.log1p(jnp.exp(-jnp.abs(v)))


def stack_rows(parts):
    return jnp.concatenate(parts, axis=0)


def kernel(nd, nm, dims, *refs):
    layers, steps, batch, width, depth, kv_cols, slots, head = dims
    rows = steps * batch
    per = nd // nm
    n_in = 22
    (
        hidden_hbm, rec_gain_hbm, in_x_hbm, in_y_hbm, conv_w_hbm, conv_b_hbm,
        gx_w_hbm, gx_b_hbm, ga_w_hbm, ga_b_hbm, decay_hbm, rec_out_hbm,
        lru_hbm, conv_s_hbm, scale_ref, attn_gain_hbm, q_w_hbm, kv_w_hbm,
        out_w_hbm, key_hbm, value_hbm, pos_ref,
    ) = refs[:n_in]
    hidden_out, lru_out, conv_out, kv_out = refs[n_in:n_in + 4]
    (
        hidden, rec_gain, in_x, in_y, conv_w, conv_b, gx_w, gx_b, ga_w, ga_b,
        decay, rec_out, lru, conv_s, attn_gain, q_w, kv_w, out_w, keys, values,
        spread_send, spread_recv, in_part, in_send, in_recv, o_part, o_send, o_recv,
        q_part, q_send, q_recv, head_send, head_recv, sum_send, sum_recv, stat_send,
        stat_recv, load_sem, spread_ss, spread_rs, part_ss, part_rs, head_ss,
        head_rs, self_sem,
    ) = refs[n_in + 4:]
    me_d = lax.axis_index("dp")
    me_m = lax.axis_index("mp")
    total = nd * nm
    me = me_d * nm + me_m

    loads = {}

    def load(name, src, dst, slot):
        copy = pltpu.make_async_copy(src, dst, load_sem.at[slot])
        copy.start()
        loads[name] = copy

    slot = 0
    for name, src, dst in (
        ("hidden", hidden_hbm, hidden), ("rec_gain", rec_gain_hbm, rec_gain),
        ("in_x0", in_x_hbm.at[0], in_x.at[0]), ("in_y0", in_y_hbm.at[0], in_y.at[0]),
        ("conv_w", conv_w_hbm, conv_w), ("conv_b", conv_b_hbm, conv_b),
        ("conv_s", conv_s_hbm, conv_s), ("lru", lru_hbm, lru),
        ("gx_b", gx_b_hbm, gx_b), ("ga_b", ga_b_hbm, ga_b), ("decay", decay_hbm, decay),
        ("gx_w", gx_w_hbm, gx_w), ("ga_w", ga_w_hbm, ga_w),
        ("rec_out0", rec_out_hbm.at[0], rec_out.at[0]),
        ("in_x1", in_x_hbm.at[1], in_x.at[1]), ("in_y1", in_y_hbm.at[1], in_y.at[1]),
        ("rec_out1", rec_out_hbm.at[1], rec_out.at[1]),
        ("attn_gain", attn_gain_hbm, attn_gain), ("q_w", q_w_hbm, q_w),
        ("kv_w", kv_w_hbm, kv_w), ("keys", key_hbm, keys), ("values", value_hbm, values),
        ("out_w", out_w_hbm, out_w),
    ):
        load(name, src, dst, slot)
        slot += 1

    barrier = pltpu.get_barrier_semaphore()

    @pl.loop(1, total)
    def _(k):
        target = lax.rem(me + k, total)
        pl.semaphore_signal(
            barrier, inc=1, device_id=(target // nm, lax.rem(target, nm)), device_id_type=MESH
        )

    pl.semaphore_wait(barrier, total - 1)

    own_slot = lax.rem(me_d, per)
    is_mine = me_d // per == me_m

    def spread(phase, block):
        for j in range(per):
            spread_send[phase, j] = block[:, j * depth:(j + 1) * depth]
        for j in range(per):
            for k in range(nm):
                target_m = lax.rem(me_m + k, nm)
                target_d = me_m * per + j
                source = spread_send.at[phase, j]

                def remote(source=source, target_d=target_d, target_m=target_m):
                    pltpu.make_async_remote_copy(
                        src_ref=source, dst_ref=spread_recv.at[phase, me_d],
                        send_sem=spread_ss.at[phase], recv_sem=spread_rs.at[phase],
                        device_id=(target_d, target_m), device_id_type=MESH,
                    ).start()

                if k == 0:
                    pl.when(target_d != me_d)(remote)
                else:
                    remote()

        @pl.when(is_mine)
        def _():
            pltpu.make_async_copy(
                spread_send.at[phase, own_slot], spread_recv.at[phase, me_d], self_sem.at[phase]
            ).start()

        @pl.when(is_mine)
        def _():
            pltpu.make_async_copy(
                spread_send.at[phase, own_slot], spread_recv.at[phase, me_d], self_sem.at[phase]
            ).wait()
            part = spread_recv.at[phase, pl.ds(0, nd - 1)]
            pltpu.make_async_copy(part, part, spread_rs.at[phase]).wait()

        @pl.when(jnp.logical_not(is_mine))
        def _():
            part = spread_recv.at[phase]
            pltpu.make_async_copy(part, part, spread_rs.at[phase]).wait()

        return spread_recv[phase].reshape(nd * rows, depth)

    def reduce_rows(sem_slot, part, send, recv, at):
        for k in range(1, nd):
            target = lax.rem(me_d + k, nd)
            send[at, k - 1] = part[pl.ds(pl.multiple_of(target * rows, rows), rows), :].astype(BF16)
            pltpu.make_async_remote_copy(
                src_ref=send.at[at, k - 1], dst_ref=recv.at[at, k - 1],
                send_sem=part_ss.at[sem_slot], recv_sem=part_rs.at[sem_slot],
                device_id=(target, me_m), device_id_type=MESH,
            ).start()
        mine = part[pl.ds(pl.multiple_of(me_d * rows, rows), rows), :]
        got = recv.at[at]
        pltpu.make_async_copy(got, got, part_rs.at[sem_slot]).wait()
        for k in range(nd - 1):
            mine = mine + recv[at, k].astype(F32)
        return mine

    def normed(gathered, gain):
        wide = gathered.astype(F32)
        squares = jnp.sum(wide * wide, axis=-1, keepdims=True)
        return (wide * gain).astype(BF16), jnp.broadcast_to(squares, (nd * rows, LANES))

    def mean_scale(squares):
        return lax.rsqrt(squares[:, :1] / float(nd * depth) + 1e-06)

    loads["hidden"].wait()
    stream = stack_rows([hidden[s].astype(F32) for s in range(steps)])

    my_block = pl.multiple_of(me_d * depth, LANES)
    for name in ("rec_gain",):
        loads[name].wait()

    for l in range(layers):
        raw = spread(2 * l, stream.astype(BF16))
        h, squares = normed(raw, rec_gain[l:l + 1, pl.ds(my_block, depth)])
        loads["in_x%d" % l].wait()
        loads["in_y%d" % l].wait()
        in_part[:, :width] = jnp.dot(h, in_x[l], preferred_element_type=F32)
        in_part[:, width:2 * width] = jnp.dot(h, in_y[l], preferred_element_type=F32)
        in_part[:, 2 * width:] = squares
        both = reduce_rows(2 * l, in_part, in_send, in_recv, l)
        scale = mean_scale(both[:, 2 * width:])
        driven = (both[:, :width] * scale).astype(BF16).astype(F32)
        gating = jax.nn.gelu(both[:, width:2 * width] * scale, approximate=True)
        if l == 0:
            for name in (
                "conv_w", "conv_b", "conv_s", "lru", "gx_b", "ga_b", "decay", "gx_w", "ga_w"
            ):
                loads[name].wait()
        taps = [conv_s[l, j].astype(F32) for j in range(conv_s.shape[1])]
        taps += [driven[s * batch:(s + 1) * batch] for s in range(steps)]
        count = conv_w.shape[1]
        filtered = conv_b[l:l + 1, :]
        for j in range(count):
            filtered = filtered + conv_w[l, j:j + 1, :] * stack_rows(taps[j:j + steps])
        for j in range(count - 1):
            conv_out[l, j] = taps[steps + j].astype(BF16)
        half = filtered.astype(BF16)
        blocks, size = gx_w.shape[1], gx_w.shape[2]
        gates = []
        for weight, bias in ((gx_w, gx_b), (ga_w, ga_b)):
            mixed = jnp.concatenate(
                [
                    jnp.dot(
                        half[:, k * size:(k + 1) * size], weight[l, k], preferred_element_type=F32
                    )
                    for k in range(blocks)
                ],
                axis=1,
            )
            gates.append(jax.nn.sigmoid(mixed + bias[l:l + 1, :]))
        log_decay = -8.0 * gates[1] * softplus(decay[l:l + 1, :])
        keep = jnp.exp(log_decay)
        add = jnp.sqrt(1.0 - jnp.exp(2.0 * log_decay)) * (gates[0] * filtered)
        index = jnp.full((1, LANES), scale_ref[l], jnp.int32).astype(F32)[:, :1]
        state_scale = jnp.exp2((index - 4.0) * 0.5)
        state = lru[l].astype(F32) * state_scale
        states = []
        for s in range(steps):
            state = keep[s * batch:(s + 1) * batch] * state + add[s * batch:(s + 1) * batch]
            states.append(state)
        lru_out[l] = (state / state_scale).astype(BF16)
        mixed = (stack_rows(states) * gating).astype(BF16)
        spreaded = spread(2 * l + 1, mixed)
        loads["rec_out%d" % l].wait()
        o_part[l] = jnp.dot(spreaded, rec_out[l], preferred_element_type=F32)
        stream = stream + reduce_rows(2 * l + 1, o_part.at[l], o_send, o_recv, l)

    raw = spread(2 * layers, stream.astype(BF16))
    loads["attn_gain"].wait()
    h, squares = normed(raw, attn_gain[:, pl.ds(my_block, depth)])
    loads["q_w"].wait()
    loads["kv_w"].wait()
    q_part[:, :width] = jnp.dot(h, q_w[...], preferred_element_type=F32)
    q_part[:, width:width + kv_cols] = jnp.dot(h, kv_w[...], preferred_element_type=F32)
    q_part[:, width + kv_cols:] = squares
    both = reduce_rows(2 * layers, q_part, q_send, q_recv, 0)
    scale = mean_scale(both[:, width + kv_cols:])
    local = (both[:, :width + kv_cols] * scale).astype(BF16)
    for s in range(steps):
        kv_out[s] = local[s * batch:(s + 1) * batch, width:]
    head_send[...] = local
    for k in range(1, nm):
        pltpu.make_async_remote_copy(
            src_ref=head_send, dst_ref=head_recv.at[me_m],
            send_sem=head_ss.at[0], recv_sem=head_rs.at[0],
            device_id=(me_d, lax.rem(me_m + k, nm)), device_id_type=MESH,
        ).start()
    head_recv[me_m] = local
    window = slots * nm
    row_ids = lax.broadcasted_iota(jnp.int32, (rows, 1), 0)
    row_seq = lax.rem(row_ids, batch)
    row_step = row_ids // batch
    position = jnp.zeros((rows, 1), jnp.int32)
    for b in range(batch):
        position = jnp.where(row_seq == b, pos_ref[b], position)
    column = lax.broadcasted_iota(jnp.int32, (rows, batch * slots), 1)
    slot_id = me_m * slots + lax.rem(column, slots)
    back = lax.rem(position - 1 - slot_id + window, window)
    held = position - 1 - back
    valid = (
        (held >= 0) & (held >= position + row_step - window + 1) & (column // slots == row_seq)
    )
    new_column = lax.broadcasted_iota(jnp.int32, (rows, rows), 1)
    new_valid = (
        (lax.rem(new_column, batch) == row_seq) & (new_column // batch <= row_step) & (me_m == 0)
    )
    loads["keys"].wait()
    loads["values"].wait()
    got = head_recv.at[pl.ds(0, nm - 1)]
    pltpu.make_async_copy(got, got, head_rs.at[0]).wait()
    group = width // head
    heads = nm * group
    query = jnp.concatenate(
        [
            head_recv[m, :, g * head:(g + 1) * head].astype(F32)
            for m in range(nm)
            for g in range(group)
        ],
        axis=0,
    ).astype(BF16)
    fresh = jnp.concatenate([head_recv[m, :, width:] for m in range(nm)], axis=1)
    factor = head ** (-0.5)
    dims_t = (((1,), (1,)), ((), ()))
    cache_keys = keys[...].reshape(batch * slots, head)
    cache_values = values[...].reshape(batch * slots, head)
    scores = lax.dot_general(query, cache_keys, dims_t, preferred_element_type=F32) * factor
    scores = scores.reshape(heads, rows, batch * slots)
    new_scores = lax.dot_general(query, fresh[:, :head], dims_t, preferred_element_type=F32)
    new_scores = (new_scores * factor).reshape(heads, rows, rows)
    scores = jnp.where(valid[None], scores, -1e30)
    new_scores = jnp.where(new_valid[None], new_scores, -1e30)
    top = jnp.maximum(
        jnp.max(scores, axis=-1, keepdims=True), jnp.max(new_scores, axis=-1, keepdims=True)
    )
    weights = jnp.where(valid[None], jnp.exp(scores - top), 0.0)
    new_weights = jnp.where(new_valid[None], jnp.exp(new_scores - top), 0.0)
    weight_sum = jnp.sum(weights, axis=-1, keepdims=True) + jnp.sum(
        new_weights, axis=-1, keepdims=True
    )
    summed = jnp.dot(
        weights.reshape(heads * rows, batch * slots).astype(BF16), cache_values,
        preferred_element_type=F32,
    ) + jnp.dot(
        new_weights.reshape(heads * rows, rows).astype(BF16), fresh[:, head:],
        preferred_element_type=F32,
    )
    top = top.reshape(heads * rows, 1)
    weight_sum = weight_sum.reshape(heads * rows, 1)
    span = group * rows
    lane = lax.broadcasted_iota(jnp.int32, (heads * rows, LANES), 1)
    stats = jnp.where(lane < LANES // 2, top, weight_sum)
    sum_send[...] = summed.astype(BF16).reshape(nm, span, head)
    stat_send[...] = stats.reshape(nm, span, LANES)
    for k in range(1, nm):
        target = lax.rem(me_m + k, nm)
        pltpu.make_async_remote_copy(
            src_ref=sum_send.at[target], dst_ref=sum_recv.at[k - 1],
            send_sem=head_ss.at[1], recv_sem=head_rs.at[1],
            device_id=(me_d, target), device_id_type=MESH,
        ).start()
        pltpu.make_async_remote_copy(
            src_ref=stat_send.at[target], dst_ref=stat_recv.at[k - 1],
            send_sem=head_ss.at[2], recv_sem=head_rs.at[2],
            device_id=(me_d, target), device_id_type=MESH,
        ).start()
    pltpu.make_async_copy(sum_recv, sum_recv, head_rs.at[1]).wait()
    pltpu.make_async_copy(stat_recv, stat_recv, head_rs.at[2]).wait()
    parts = [(sum_send[me_m], stat_send[me_m])]
    parts += [(sum_recv[k], stat_recv[k]) for k in range(nm - 1)]
    tops = [stat[:, :1] for _, stat in parts]
    best = functools.reduce(jnp.maximum, tops)
    fades = [jnp.exp(t - best) for t in tops]
    whole = sum(f * stat[:, LANES // 2:LANES // 2 + 1] for f, (_, stat) in zip(fades, parts))
    mixed = sum(f * part.astype(F32) for f, (part, _) in zip(fades, parts)) / whole
    attended = jnp.concatenate(
        [mixed[g * rows:(g + 1) * rows] for g in range(group)], axis=1
    ).astype(BF16)
    spreaded = spread(2 * layers + 1, attended)
    loads["out_w"].wait()
    o_part[layers] = jnp.dot(spreaded, out_w[...], preferred_element_type=F32)
    stream = stream + reduce_rows(2 * layers + 1, o_part.at[layers], o_send, o_recv, layers)
    for s in range(steps):
        hidden_out[s] = stream[s * batch:(s + 1) * batch].astype(BF16)

    for phase in range(2 * layers + 2):
        @pl.when(is_mine)
        def _(phase=phase):
            part = spread_recv.at[phase, pl.ds(0, nd - 1)]
            pltpu.make_async_copy(part, part, spread_ss.at[phase]).wait()

        @pl.when(jnp.logical_not(is_mine))
        def _(phase=phase):
            part = spread_recv.at[phase]
            pltpu.make_async_copy(part, part, spread_ss.at[phase]).wait()

    for l in range(layers):
        for sem_slot, ref in ((2 * l, in_send), (2 * l + 1, o_send)):
            pltpu.make_async_copy(ref.at[l], ref.at[l], part_ss.at[sem_slot]).wait()
    pltpu.make_async_copy(q_send.at[0], q_send.at[0], part_ss.at[2 * layers]).wait()
    pltpu.make_async_copy(o_send.at[layers], o_send.at[layers], part_ss.at[2 * layers + 1]).wait()
    got = head_recv.at[pl.ds(0, nm - 1)]
    pltpu.make_async_copy(got, got, head_ss.at[0]).wait()
    pltpu.make_async_copy(sum_recv, sum_recv, head_ss.at[1]).wait()
    pltpu.make_async_copy(stat_recv, stat_recv, head_ss.at[2]).wait()


def body(nd, nm, *args):
    (
        hidden_in, rec_gain, in_x, in_y, conv_w, conv_b, gx_w, gx_b, ga_w, ga_b, decay,
        rec_out, lru, conv_s, scale_index, attn_gain, q_w, kv_w, out_w, keys, values, positions,
    ) = args
    steps, batch, width = hidden_in.shape
    layers, depth = in_x.shape[:2]
    kv_cols = kv_w.shape[1]
    slots, head = keys.shape[1:]
    rows = steps * batch
    per = nd // nm
    group = width // head
    span = group * rows
    dims = (layers, steps, batch, width, depth, kv_cols, slots, head)
    attn_gain = attn_gain.reshape(1, -1)
    args = (
        hidden_in, rec_gain, in_x, in_y, conv_w, conv_b, gx_w, gx_b, ga_w, ga_b, decay,
        rec_out, lru, conv_s, scale_index, attn_gain, q_w, kv_w, out_w, keys, values, positions,
    )
    in_smem = (14, 21)
    in_cols = 2 * width + LANES
    q_cols = width + kv_cols + LANES
    phases = 2 * layers + 2
    held = [
        pltpu.VMEM(a.shape, a.dtype) for i, a in enumerate(args) if i not in in_smem
    ]
    any_spec = pl.BlockSpec(memory_space=pl.ANY)
    smem = pl.BlockSpec(memory_space=pltpu.SMEM)
    vmem = pl.BlockSpec(memory_space=pltpu.VMEM)
    return pl.pallas_call(
        functools.partial(kernel, nd, nm, dims),
        out_shape=(
            jax.ShapeDtypeStruct(hidden_in.shape, BF16),
            jax.ShapeDtypeStruct(lru.shape, BF16),
            jax.ShapeDtypeStruct(conv_s.shape, BF16),
            jax.ShapeDtypeStruct((steps, batch, kv_cols), BF16),
        ),
        in_specs=[smem if i in in_smem else any_spec for i in range(len(args))],
        out_specs=(vmem,) * 4,
        scratch_shapes=held + [
            pltpu.VMEM((phases, per, rows, depth), BF16),
            pltpu.VMEM((phases, nd, rows, depth), BF16),
            pltpu.VMEM((nd * rows, in_cols), F32),
            pltpu.VMEM((layers, nd - 1, rows, in_cols), BF16),
            pltpu.VMEM((layers, nd - 1, rows, in_cols), BF16),
            pltpu.VMEM((layers + 1, nd * rows, width), F32),
            pltpu.VMEM((layers + 1, nd - 1, rows, width), BF16),
            pltpu.VMEM((layers + 1, nd - 1, rows, width), BF16),
            pltpu.VMEM((nd * rows, q_cols), F32),
            pltpu.VMEM((1, nd - 1, rows, q_cols), BF16),
            pltpu.VMEM((1, nd - 1, rows, q_cols), BF16),
            pltpu.VMEM((rows, width + kv_cols), BF16),
            pltpu.VMEM((nm, rows, width + kv_cols), BF16),
            pltpu.VMEM((nm, span, head), BF16),
            pltpu.VMEM((nm - 1, span, head), BF16),
            pltpu.VMEM((nm, span, LANES), F32),
            pltpu.VMEM((nm - 1, span, LANES), F32),
            pltpu.SemaphoreType.DMA((23,)),
            pltpu.SemaphoreType.DMA((phases,)),
            pltpu.SemaphoreType.DMA((phases,)),
            pltpu.SemaphoreType.DMA((phases,)),
            pltpu.SemaphoreType.DMA((phases,)),
            pltpu.SemaphoreType.DMA((3,)),
            pltpu.SemaphoreType.DMA((3,)),
            pltpu.SemaphoreType.DMA((phases,)),
        ],
        compiler_params=pltpu.CompilerParams(
            collective_id=0, has_side_effects=True, vmem_limit_bytes=56 * 1024 * 1024
        ),
    )(*args)


def solution(mesh):
    placed = (
        P(None, "dp", "mp"),
        P(),
        P(None, "dp", "mp"),
        P(None, "dp", "mp"),
        P(None, None, "mp"),
        P(None, "mp"),
        P(None, "mp", None, None),
        P(None, "mp"),
        P(None, "mp", None, None),
        P(None, "mp"),
        P(None, "mp"),
        P(None, "dp", "mp"),
        P(None, "dp", "mp"),
        P(None, None, "dp", "mp"),
        P(),
        P(),
        P("dp", "mp"),
        P("dp", "mp"),
        P("dp", "mp"),
        P("dp", "mp", None),
        P("dp", "mp", None),
        P("dp"),
    )
    return jax.shard_map(
        functools.partial(body, mesh.shape["dp"], mesh.shape["mp"]),
        mesh=mesh,
        in_specs=placed,
        out_specs=(
            P(None, "dp", "mp"),
            P(None, "dp", "mp"),
            P(None, None, "dp", "mp"),
            P(None, "dp", "mp"),
        ),
        check_vma=False,
    )
```

```python
import functools

import jax
import jax.numpy as jnp
from jax import lax
from jax.experimental import pallas as pl
from jax.experimental.pallas import tpu as pltpu
from jax.sharding import PartitionSpec as P

MESH = pl.DeviceIdType.MESH
LANES = 128
F32 = jnp.float32
BF16 = jnp.bfloat16


def softplus(v):
    return jnp.maximum(v, 0.0) + jnp.log1p(jnp.exp(-jnp.abs(v)))


def stack_rows(parts):
    return jnp.concatenate(parts, axis=0)


def kernel(nd, nm, dims, *refs):
    layers, steps, batch, width, depth, kv_cols, slots, head = dims
    rows = steps * batch
    per = nd // nm
    n_in = 22
    (
        hidden_hbm, rec_gain_hbm, in_x_hbm, in_y_hbm, conv_w_hbm, conv_b_hbm,
        gx_w_hbm, gx_b_hbm, ga_w_hbm, ga_b_hbm, decay_hbm, rec_out_hbm,
        lru_hbm, conv_s_hbm, scale_ref, attn_gain_hbm, q_w_hbm, kv_w_hbm,
        out_w_hbm, key_hbm, value_hbm, pos_ref,
    ) = refs[:n_in]
    hidden_out, lru_out, conv_out, kv_out = refs[n_in:n_in + 4]
    (
        hidden, rec_gain, in_x, in_y, conv_w, conv_b, gx_w, gx_b, ga_w, ga_b,
        decay, rec_out, lru, conv_s, attn_gain, q_w, kv_w, out_w, keys, values,
        spread_send, spread_recv, in_part, in_send, in_recv, o_part, o_send, o_recv,
        q_part, q_send, q_recv, head_send, head_recv, sum_send, sum_recv, stat_send,
        stat_recv, load_sem, spread_ss, spread_rs, part_ss, part_rs, head_ss,
        head_rs, self_sem,
    ) = refs[n_in + 4:]
    me_d = lax.axis_index("dp")
    me_m = lax.axis_index("mp")
    total = nd * nm
    me = me_d * nm + me_m

    loads = {}

    def load(name, src, dst, slot):
        copy = pltpu.make_async_copy(src, dst, load_sem.at[slot])
        copy.start()
        loads[name] = copy

    slot = 0
    for name, src, dst in (
        ("hidden", hidden_hbm, hidden), ("rec_gain", rec_gain_hbm, rec_gain),
        ("in_x0", in_x_hbm.at[0], in_x.at[0]), ("in_y0", in_y_hbm.at[0], in_y.at[0]),
        ("conv_w", conv_w_hbm, conv_w), ("conv_b", conv_b_hbm, conv_b),
        ("conv_s", conv_s_hbm, conv_s), ("lru", lru_hbm, lru),
        ("gx_b", gx_b_hbm, gx_b), ("ga_b", ga_b_hbm, ga_b), ("decay", decay_hbm, decay),
        ("gx_w", gx_w_hbm, gx_w), ("ga_w", ga_w_hbm, ga_w),
        ("rec_out0", rec_out_hbm.at[0], rec_out.at[0]),
        ("in_x1", in_x_hbm.at[1], in_x.at[1]), ("in_y1", in_y_hbm.at[1], in_y.at[1]),
        ("rec_out1", rec_out_hbm.at[1], rec_out.at[1]),
        ("attn_gain", attn_gain_hbm, attn_gain), ("q_w", q_w_hbm, q_w),
        ("kv_w", kv_w_hbm, kv_w), ("keys", key_hbm, keys), ("values", value_hbm, values),
        ("out_w", out_w_hbm, out_w),
    ):
        load(name, src, dst, slot)
        slot += 1

    barrier = pltpu.get_barrier_semaphore()

    @pl.loop(1, total)
    def _(k):
        target = lax.rem(me + k, total)
        pl.semaphore_signal(
            barrier, inc=1, device_id=(target // nm, lax.rem(target, nm)), device_id_type=MESH
        )

    pl.semaphore_wait(barrier, total - 1)

    own_slot = lax.rem(me_d, per)
    is_mine = me_d // per == me_m

    def spread(phase, block):
        for j in range(per):
            spread_send[phase, j] = block[:, j * depth:(j + 1) * depth]
        for j in range(per):
            for k in range(nm):
                target_m = lax.rem(me_m + k, nm)
                target_d = me_m * per + j
                source = spread_send.at[phase, j]

                def remote(source=source, target_d=target_d, target_m=target_m):
                    pltpu.make_async_remote_copy(
                        src_ref=source, dst_ref=spread_recv.at[phase, me_d],
                        send_sem=spread_ss.at[phase], recv_sem=spread_rs.at[phase],
                        device_id=(target_d, target_m), device_id_type=MESH,
                    ).start()

                if k == 0:
                    pl.when(target_d != me_d)(remote)
                else:
                    remote()

        @pl.when(is_mine)
        def _():
            pltpu.make_async_copy(
                spread_send.at[phase, own_slot], spread_recv.at[phase, me_d], self_sem.at[phase]
            ).start()

        @pl.when(is_mine)
        def _():
            pltpu.make_async_copy(
                spread_send.at[phase, own_slot], spread_recv.at[phase, me_d], self_sem.at[phase]
            ).wait()
            part = spread_recv.at[phase, pl.ds(0, nd - 1)]
            pltpu.make_async_copy(part, part, spread_rs.at[phase]).wait()

        @pl.when(jnp.logical_not(is_mine))
        def _():
            part = spread_recv.at[phase]
            pltpu.make_async_copy(part, part, spread_rs.at[phase]).wait()

        return spread_recv[phase].reshape(nd * rows, depth)

    def reduce_rows(sem_slot, part, send, recv, at):
        for k in range(1, nd):
            target = lax.rem(me_d + k, nd)
            send[at, k - 1] = part[pl.ds(pl.multiple_of(target * rows, rows), rows), :].astype(BF16)
            pltpu.make_async_remote_copy(
                src_ref=send.at[at, k - 1], dst_ref=recv.at[at, k - 1],
                send_sem=part_ss.at[sem_slot], recv_sem=part_rs.at[sem_slot],
                device_id=(target, me_m), device_id_type=MESH,
            ).start()
        mine = part[pl.ds(pl.multiple_of(me_d * rows, rows), rows), :]
        got = recv.at[at]
        pltpu.make_async_copy(got, got, part_rs.at[sem_slot]).wait()
        for k in range(nd - 1):
            mine = mine + recv[at, k].astype(F32)
        return mine

    def normed(gathered, gain):
        wide = gathered.astype(F32)
        squares = jnp.sum(wide * wide, axis=-1, keepdims=True)
        return (wide * gain).astype(BF16), jnp.broadcast_to(squares, (nd * rows, LANES))

    def mean_scale(squares):
        return lax.rsqrt(squares[:, :1] / float(nd * depth) + 1e-06)

    loads["hidden"].wait()
    stream = stack_rows([hidden[s].astype(F32) for s in range(steps)])

    my_block = pl.multiple_of(me_d * depth, LANES)
    for name in ("rec_gain",):
        loads[name].wait()

    for l in range(layers):
        raw = spread(2 * l, stream.astype(BF16))
        h, squares = normed(raw, rec_gain[l:l + 1, pl.ds(my_block, depth)])
        loads["in_x%d" % l].wait()
        loads["in_y%d" % l].wait()
        in_part[:, :width] = jnp.dot(h, in_x[l], preferred_element_type=F32)
        in_part[:, width:2 * width] = jnp.dot(h, in_y[l], preferred_element_type=F32)
        in_part[:, 2 * width:] = squares
        both = reduce_rows(2 * l, in_part, in_send, in_recv, l)
        scale = mean_scale(both[:, 2 * width:])
        driven = (both[:, :width] * scale).astype(BF16).astype(F32)
        gating = jax.nn.gelu(both[:, width:2 * width] * scale, approximate=True)
        if l == 0:
            for name in (
                "conv_w", "conv_b", "conv_s", "lru", "gx_b", "ga_b", "decay", "gx_w", "ga_w"
            ):
                loads[name].wait()
        taps = [conv_s[l, j].astype(F32) for j in range(conv_s.shape[1])]
        taps += [driven[s * batch:(s + 1) * batch] for s in range(steps)]
        count = conv_w.shape[1]
        filtered = conv_b[l:l + 1, :]
        for j in range(count):
            filtered = filtered + conv_w[l, j:j + 1, :] * stack_rows(taps[j:j + steps])
        for j in range(count - 1):
            conv_out[l, j] = taps[steps + j].astype(BF16)
        half = filtered.astype(BF16)
        blocks, size = gx_w.shape[1], gx_w.shape[2]
        gates = []
        for weight, bias in ((gx_w, gx_b), (ga_w, ga_b)):
            mixed = jnp.concatenate(
                [
                    jnp.dot(
                        half[:, k * size:(k + 1) * size], weight[l, k], preferred_element_type=F32
                    )
                    for k in range(blocks)
                ],
                axis=1,
            )
            gates.append(jax.nn.sigmoid(mixed + bias[l:l + 1, :]))
        log_decay = -8.0 * gates[1] * softplus(decay[l:l + 1, :])
        keep = jnp.exp(log_decay)
        add = jnp.sqrt(1.0 - jnp.exp(2.0 * log_decay)) * (gates[0] * filtered)
        index = jnp.full((1, LANES), scale_ref[l], jnp.int32).astype(F32)[:, :1]
        state_scale = jnp.exp2((index - 4.0) * 0.5)
        state = lru[l].astype(F32) * state_scale
        states = []
        for s in range(steps):
            state = keep[s * batch:(s + 1) * batch] * state + add[s * batch:(s + 1) * batch]
            states.append(state)
        lru_out[l] = (state / state_scale).astype(BF16)
        mixed = (stack_rows(states) * gating).astype(BF16)
        spreaded = spread(2 * l + 1, mixed)
        loads["rec_out%d" % l].wait()
        o_part[l] = jnp.dot(spreaded, rec_out[l], preferred_element_type=F32)
        stream = stream + reduce_rows(2 * l + 1, o_part.at[l], o_send, o_recv, l)

    raw = spread(2 * layers, stream.astype(BF16))
    loads["attn_gain"].wait()
    h, squares = normed(raw, attn_gain[:, pl.ds(my_block, depth)])
    loads["q_w"].wait()
    loads["kv_w"].wait()
    q_part[:, :width] = jnp.dot(h, q_w[...], preferred_element_type=F32)
    q_part[:, width:width + kv_cols] = jnp.dot(h, kv_w[...], preferred_element_type=F32)
    q_part[:, width + kv_cols:] = squares
    both = reduce_rows(2 * layers, q_part, q_send, q_recv, 0)
    scale = mean_scale(both[:, width + kv_cols:])
    local = (both[:, :width + kv_cols] * scale).astype(BF16)
    for s in range(steps):
        kv_out[s] = local[s * batch:(s + 1) * batch, width:]
    head_send[...] = local
    for k in range(1, nm):
        pltpu.make_async_remote_copy(
            src_ref=head_send, dst_ref=head_recv.at[me_m],
            send_sem=head_ss.at[0], recv_sem=head_rs.at[0],
            device_id=(me_d, lax.rem(me_m + k, nm)), device_id_type=MESH,
        ).start()
    head_recv[me_m] = local
    window = slots * nm
    row_ids = lax.broadcasted_iota(jnp.int32, (rows, 1), 0)
    row_seq = lax.rem(row_ids, batch)
    row_step = row_ids // batch
    position = jnp.zeros((rows, 1), jnp.int32)
    for b in range(batch):
        position = jnp.where(row_seq == b, pos_ref[b], position)
    column = lax.broadcasted_iota(jnp.int32, (rows, batch * slots), 1)
    slot_id = me_m * slots + lax.rem(column, slots)
    back = lax.rem(position - 1 - slot_id + window, window)
    held = position - 1 - back
    valid = (
        (held >= 0) & (held >= position + row_step - window + 1) & (column // slots == row_seq)
    )
    new_column = lax.broadcasted_iota(jnp.int32, (rows, rows), 1)
    new_valid = (
        (lax.rem(new_column, batch) == row_seq) & (new_column // batch <= row_step) & (me_m == 0)
    )
    loads["keys"].wait()
    loads["values"].wait()
    got = head_recv.at[pl.ds(0, nm - 1)]
    pltpu.make_async_copy(got, got, head_rs.at[0]).wait()
    group = width // head
    heads = nm * group
    query = jnp.concatenate(
        [
            head_recv[m, :, g * head:(g + 1) * head].astype(F32)
            for m in range(nm)
            for g in range(group)
        ],
        axis=0,
    ).astype(BF16)
    fresh = jnp.concatenate([head_recv[m, :, width:] for m in range(nm)], axis=1)
    factor = head ** (-0.5)
    dims_t = (((1,), (1,)), ((), ()))
    cache_keys = keys[...].reshape(batch * slots, head)
    cache_values = values[...].reshape(batch * slots, head)
    scores = lax.dot_general(query, cache_keys, dims_t, preferred_element_type=F32) * factor
    scores = scores.reshape(heads, rows, batch * slots)
    new_scores = lax.dot_general(query, fresh[:, :head], dims_t, preferred_element_type=F32)
    new_scores = (new_scores * factor).reshape(heads, rows, rows)
    scores = jnp.where(valid[None], scores, -1e30)
    new_scores = jnp.where(new_valid[None], new_scores, -1e30)
    top = jnp.maximum(
        jnp.max(scores, axis=-1, keepdims=True), jnp.max(new_scores, axis=-1, keepdims=True)
    )
    weights = jnp.where(valid[None], jnp.exp(scores - top), 0.0)
    new_weights = jnp.where(new_valid[None], jnp.exp(new_scores - top), 0.0)
    weight_sum = jnp.sum(weights, axis=-1, keepdims=True) + jnp.sum(
        new_weights, axis=-1, keepdims=True
    )
    summed = jnp.dot(
        weights.reshape(heads * rows, batch * slots).astype(BF16), cache_values,
        preferred_element_type=F32,
    ) + jnp.dot(
        new_weights.reshape(heads * rows, rows).astype(BF16), fresh[:, head:],
        preferred_element_type=F32,
    )
    top = top.reshape(heads * rows, 1)
    weight_sum = weight_sum.reshape(heads * rows, 1)
    span = group * rows
    lane = lax.broadcasted_iota(jnp.int32, (heads * rows, LANES), 1)
    stats = jnp.where(lane < LANES // 2, top, weight_sum)
    sum_send[...] = summed.astype(BF16).reshape(nm, span, head)
    stat_send[...] = stats.reshape(nm, span, LANES)
    for k in range(1, nm):
        target = lax.rem(me_m + k, nm)
        pltpu.make_async_remote_copy(
            src_ref=sum_send.at[target], dst_ref=sum_recv.at[k - 1],
            send_sem=head_ss.at[1], recv_sem=head_rs.at[1],
            device_id=(me_d, target), device_id_type=MESH,
        ).start()
        pltpu.make_async_remote_copy(
            src_ref=stat_send.at[target], dst_ref=stat_recv.at[k - 1],
            send_sem=head_ss.at[2], recv_sem=head_rs.at[2],
            device_id=(me_d, target), device_id_type=MESH,
        ).start()
    pltpu.make_async_copy(sum_recv, sum_recv, head_rs.at[1]).wait()
    pltpu.make_async_copy(stat_recv, stat_recv, head_rs.at[2]).wait()
    parts = [(sum_send[me_m], stat_send[me_m])]
    parts += [(sum_recv[k], stat_recv[k]) for k in range(nm - 1)]
    tops = [stat[:, :1] for _, stat in parts]
    best = functools.reduce(jnp.maximum, tops)
    fades = [jnp.exp(t - best) for t in tops]
    whole = sum(f * stat[:, LANES // 2:LANES // 2 + 1] for f, (_, stat) in zip(fades, parts))
    mixed = sum(f * part.astype(F32) for f, (part, _) in zip(fades, parts)) / whole
    attended = jnp.concatenate(
        [mixed[g * rows:(g + 1) * rows] for g in range(group)], axis=1
    ).astype(BF16)
    spreaded = spread(2 * layers + 1, attended)
    loads["out_w"].wait()
    o_part[layers] = jnp.dot(spreaded, out_w[...], preferred_element_type=F32)
    stream = stream + reduce_rows(2 * layers + 1, o_part.at[layers], o_send, o_recv, layers)
    for s in range(steps):
        hidden_out[s] = stream[s * batch:(s + 1) * batch].astype(BF16)

    for phase in range(2 * layers + 2):
        @pl.when(is_mine)
        def _(phase=phase):
            part = spread_recv.at[phase, pl.ds(0, nd - 1)]
            pltpu.make_async_copy(part, part, spread_ss.at[phase]).wait()

        @pl.when(jnp.logical_not(is_mine))
        def _(phase=phase):
            part = spread_recv.at[phase]
            pltpu.make_async_copy(part, part, spread_ss.at[phase]).wait()

    for l in range(layers):
        for sem_slot, ref in ((2 * l, in_send), (2 * l + 1, o_send)):
            pltpu.make_async_copy(ref.at[l], ref.at[l], part_ss.at[sem_slot]).wait()
    pltpu.make_async_copy(q_send.at[0], q_send.at[0], part_ss.at[2 * layers]).wait()
    pltpu.make_async_copy(o_send.at[layers], o_send.at[layers], part_ss.at[2 * layers + 1]).wait()
    got = head_recv.at[pl.ds(0, nm - 1)]
    pltpu.make_async_copy(got, got, head_ss.at[0]).wait()
    pltpu.make_async_copy(sum_recv, sum_recv, head_ss.at[1]).wait()
    pltpu.make_async_copy(stat_recv, stat_recv, head_ss.at[2]).wait()


def put_out(*refs):
    copies = [
        pltpu.make_async_copy(refs[i], refs[4 + i], refs[8].at[i]) for i in range(4)
    ]
    for copy in copies:
        copy.start()
    for copy in copies:
        copy.wait()


def body(nd, nm, *args):
    (
        hidden_in, rec_gain, in_x, in_y, conv_w, conv_b, gx_w, gx_b, ga_w, ga_b, decay,
        rec_out, lru, conv_s, scale_index, attn_gain, q_w, kv_w, out_w, keys, values, positions,
    ) = args
    steps, batch, width = hidden_in.shape
    layers, depth = in_x.shape[:2]
    kv_cols = kv_w.shape[1]
    slots, head = keys.shape[1:]
    rows = steps * batch
    per = nd // nm
    group = width // head
    span = group * rows
    dims = (layers, steps, batch, width, depth, kv_cols, slots, head)
    attn_gain = attn_gain.reshape(1, -1)
    args = (
        hidden_in, rec_gain, in_x, in_y, conv_w, conv_b, gx_w, gx_b, ga_w, ga_b, decay,
        rec_out, lru, conv_s, scale_index, attn_gain, q_w, kv_w, out_w, keys, values, positions,
    )
    in_smem = (14, 21)
    in_cols = 2 * width + LANES
    q_cols = width + kv_cols + LANES
    phases = 2 * layers + 2
    held = [
        pltpu.VMEM(a.shape, a.dtype) for i, a in enumerate(args) if i not in in_smem
    ]
    any_spec = pl.BlockSpec(memory_space=pl.ANY)
    smem = pl.BlockSpec(memory_space=pltpu.SMEM)
    vmem = pl.BlockSpec(memory_space=pltpu.VMEM)
    shapes = (hidden_in.shape, lru.shape, conv_s.shape, (steps, batch, kv_cols))
    results = pl.pallas_call(
        functools.partial(kernel, nd, nm, dims),
        out_shape=tuple(pltpu.VMEM(shape, BF16) for shape in shapes),
        in_specs=[smem if i in in_smem else any_spec for i in range(len(args))],
        out_specs=(vmem,) * 4,
        scratch_shapes=held + [
            pltpu.VMEM((phases, per, rows, depth), BF16),
            pltpu.VMEM((phases, nd, rows, depth), BF16),
            pltpu.VMEM((nd * rows, in_cols), F32),
            pltpu.VMEM((layers, nd - 1, rows, in_cols), BF16),
            pltpu.VMEM((layers, nd - 1, rows, in_cols), BF16),
            pltpu.VMEM((layers + 1, nd * rows, width), F32),
            pltpu.VMEM((layers + 1, nd - 1, rows, width), BF16),
            pltpu.VMEM((layers + 1, nd - 1, rows, width), BF16),
            pltpu.VMEM((nd * rows, q_cols), F32),
            pltpu.VMEM((1, nd - 1, rows, q_cols), BF16),
            pltpu.VMEM((1, nd - 1, rows, q_cols), BF16),
            pltpu.VMEM((rows, width + kv_cols), BF16),
            pltpu.VMEM((nm, rows, width + kv_cols), BF16),
            pltpu.VMEM((nm, span, head), BF16),
            pltpu.VMEM((nm - 1, span, head), BF16),
            pltpu.VMEM((nm, span, LANES), F32),
            pltpu.VMEM((nm - 1, span, LANES), F32),
            pltpu.SemaphoreType.DMA((23,)),
            pltpu.SemaphoreType.DMA((phases,)),
            pltpu.SemaphoreType.DMA((phases,)),
            pltpu.SemaphoreType.DMA((phases,)),
            pltpu.SemaphoreType.DMA((phases,)),
            pltpu.SemaphoreType.DMA((3,)),
            pltpu.SemaphoreType.DMA((3,)),
            pltpu.SemaphoreType.DMA((phases,)),
        ],
        compiler_params=pltpu.CompilerParams(
            collective_id=0, has_side_effects=True, vmem_limit_bytes=56 * 1024 * 1024
        ),
    )(*args)
    return pl.pallas_call(
        put_out,
        out_shape=tuple(jax.ShapeDtypeStruct(shape, BF16) for shape in shapes),
        in_specs=[vmem] * 4,
        out_specs=(any_spec,) * 4,
        scratch_shapes=[pltpu.SemaphoreType.DMA((4,))],
        compiler_params=pltpu.CompilerParams(vmem_limit_bytes=1024 * 1024),
    )(*results)


def solution(mesh):
    placed = (
        P(None, "dp", "mp"),
        P(),
        P(None, "dp", "mp"),
        P(None, "dp", "mp"),
        P(None, None, "mp"),
        P(None, "mp"),
        P(None, "mp", None, None),
        P(None, "mp"),
        P(None, "mp", None, None),
        P(None, "mp"),
        P(None, "mp"),
        P(None, "dp", "mp"),
        P(None, "dp", "mp"),
        P(None, None, "dp", "mp"),
        P(),
        P(),
        P("dp", "mp"),
        P("dp", "mp"),
        P("dp", "mp"),
        P("dp", "mp", None),
        P("dp", "mp", None),
        P("dp"),
    )
    return jax.shard_map(
        functools.partial(body, mesh.shape["dp"], mesh.shape["mp"]),
        mesh=mesh,
        in_specs=placed,
        out_specs=(
            P(None, "dp", "mp"),
            P(None, "dp", "mp"),
            P(None, None, "dp", "mp"),
            P(None, "dp", "mp"),
        ),
        check_vma=False,
    )
```

```python
import functools

import jax
import jax.numpy as jnp
from jax import lax
from jax.experimental import pallas as pl
from jax.experimental.pallas import tpu as pltpu
from jax.sharding import PartitionSpec as P

MESH = pl.DeviceIdType.MESH
LANES = 128
F32 = jnp.float32
BF16 = jnp.bfloat16


def softplus(v):
    return jnp.maximum(v, 0.0) + jnp.log1p(jnp.exp(-jnp.abs(v)))


def stack_rows(parts):
    return jnp.concatenate(parts, axis=0)


def kernel(nd, nm, dims, *refs):
    layers, steps, batch, width, depth, kv_cols, slots, head = dims
    rows = steps * batch
    per = nd // nm
    n_in = 22
    (
        hidden_hbm, rec_gain_hbm, in_x_hbm, in_y_hbm, conv_w_hbm, conv_b_hbm,
        gx_w_hbm, gx_b_hbm, ga_w_hbm, ga_b_hbm, decay_hbm, rec_out_hbm,
        lru_hbm, conv_s_hbm, scale_ref, attn_gain_hbm, q_w_hbm, kv_w_hbm,
        out_w_hbm, key_hbm, value_hbm, pos_ref,
    ) = refs[:n_in]
    hidden_out, lru_out, conv_out, kv_out = refs[n_in:n_in + 4]
    (
        hidden, rec_gain, in_x, in_y, conv_w, conv_b, gx_w, gx_b, ga_w, ga_b,
        decay, rec_out, lru, conv_s, attn_gain, q_w, kv_w, out_w, keys, values,
        spread_send, spread_recv, in_part, in_send, in_recv, o_part, o_send, o_recv,
        q_part, q_send, q_recv, head_send, head_recv, sum_send, sum_recv, stat_send,
        stat_recv, load_sem, spread_ss, spread_rs, part_ss, part_rs, head_ss,
        head_rs, self_sem,
    ) = refs[n_in + 4:]
    me_d = lax.axis_index("dp")
    me_m = lax.axis_index("mp")
    own_slot = lax.rem(me_d, per)
    is_mine = me_d // per == me_m

    barrier = pltpu.get_barrier_semaphore()

    def greet(target_d, target_m):
        pl.semaphore_signal(
            barrier, inc=1, device_id=(target_d, target_m), device_id_type=MESH
        )

    for k in range(nd):
        source_d = lax.rem(me_d + k, nd)
        if k == 0:
            pl.when(jnp.logical_not(is_mine))(lambda: greet(me_d, me_d // per))
        else:
            greet(source_d, me_d // per)
            greet(source_d, me_m)
    for k in range(1, nm):
        greet(me_d, lax.rem(me_m + k, nm))

    loads = {}

    def load(name, src, dst, slot):
        copy = pltpu.make_async_copy(src, dst, load_sem.at[slot])
        copy.start()
        loads[name] = copy

    slot = 0
    for name, src, dst in (
        ("hidden", hidden_hbm, hidden), ("rec_gain", rec_gain_hbm, rec_gain),
        ("in_x0", in_x_hbm.at[0], in_x.at[0]), ("in_y0", in_y_hbm.at[0], in_y.at[0]),
        ("conv_w", conv_w_hbm, conv_w), ("conv_b", conv_b_hbm, conv_b),
        ("conv_s", conv_s_hbm, conv_s), ("lru", lru_hbm, lru),
        ("gx_b", gx_b_hbm, gx_b), ("ga_b", ga_b_hbm, ga_b), ("decay", decay_hbm, decay),
        ("gx_w", gx_w_hbm, gx_w), ("ga_w", ga_w_hbm, ga_w),
        ("rec_out0", rec_out_hbm.at[0], rec_out.at[0]),
        ("in_x1", in_x_hbm.at[1], in_x.at[1]), ("in_y1", in_y_hbm.at[1], in_y.at[1]),
        ("rec_out1", rec_out_hbm.at[1], rec_out.at[1]),
        ("attn_gain", attn_gain_hbm, attn_gain), ("q_w", q_w_hbm, q_w),
        ("kv_w", kv_w_hbm, kv_w), ("keys", key_hbm, keys), ("values", value_hbm, values),
        ("out_w", out_w_hbm, out_w),
    ):
        load(name, src, dst, slot)
        slot += 1

    @pl.when(is_mine)
    def _():
        pl.semaphore_wait(barrier, 2 * nd + nm - 3)

    @pl.when(jnp.logical_not(is_mine))
    def _():
        pl.semaphore_wait(barrier, 2 * nd + nm - 2)

    def spread(phase, block):
        for j in range(per):
            spread_send[phase, j] = block[:, j * depth:(j + 1) * depth]
        for j in range(per):
            for k in range(nm):
                target_m = lax.rem(me_m + k, nm)
                target_d = me_m * per + j
                source = spread_send.at[phase, j]

                def remote(source=source, target_d=target_d, target_m=target_m):
                    pltpu.make_async_remote_copy(
                        src_ref=source, dst_ref=spread_recv.at[phase, me_d],
                        send_sem=spread_ss.at[phase], recv_sem=spread_rs.at[phase],
                        device_id=(target_d, target_m), device_id_type=MESH,
                    ).start()

                if k == 0:
                    pl.when(target_d != me_d)(remote)
                else:
                    remote()

        @pl.when(is_mine)
        def _():
            pltpu.make_async_copy(
                spread_send.at[phase, own_slot], spread_recv.at[phase, me_d], self_sem.at[phase]
            ).start()

        @pl.when(is_mine)
        def _():
            pltpu.make_async_copy(
                spread_send.at[phase, own_slot], spread_recv.at[phase, me_d], self_sem.at[phase]
            ).wait()
            part = spread_recv.at[phase, pl.ds(0, nd - 1)]
            pltpu.make_async_copy(part, part, spread_rs.at[phase]).wait()

        @pl.when(jnp.logical_not(is_mine))
        def _():
            part = spread_recv.at[phase]
            pltpu.make_async_copy(part, part, spread_rs.at[phase]).wait()

        return spread_recv[phase].reshape(nd * rows, depth)

    def send_rows(sem_slot, part, send, recv, at):
        for k in range(1, nd):
            target = lax.rem(me_d + k, nd)
            send[at, k - 1] = part[pl.ds(pl.multiple_of(target * rows, rows), rows), :].astype(BF16)
            pltpu.make_async_remote_copy(
                src_ref=send.at[at, k - 1], dst_ref=recv.at[at, k - 1],
                send_sem=part_ss.at[sem_slot], recv_sem=part_rs.at[sem_slot],
                device_id=(target, me_m), device_id_type=MESH,
            ).start()

    def reduced(sem_slot, part, recv, at):
        mine = part[pl.ds(pl.multiple_of(me_d * rows, rows), rows), :]
        got = recv.at[at]
        pltpu.make_async_copy(got, got, part_rs.at[sem_slot]).wait()
        for k in range(nd - 1):
            mine = mine + recv[at, k].astype(F32)
        return mine

    def normed(gathered, gain):
        wide = gathered.astype(F32)
        squares = jnp.sum(wide * wide, axis=-1, keepdims=True)
        return (wide * gain).astype(BF16), jnp.broadcast_to(squares, (nd * rows, LANES))

    def mean_scale(squares):
        return lax.rsqrt(squares[:, :1] / float(nd * depth) + 1e-06)

    loads["hidden"].wait()
    stream = stack_rows([hidden[s].astype(F32) for s in range(steps)])

    my_block = pl.multiple_of(me_d * depth, LANES)
    for name in ("rec_gain",):
        loads[name].wait()

    for l in range(layers):
        raw = spread(2 * l, stream.astype(BF16))
        h, squares = normed(raw, rec_gain[l:l + 1, pl.ds(my_block, depth)])
        loads["in_x%d" % l].wait()
        in_part[:, :width] = jnp.dot(h, in_x[l], preferred_element_type=F32)
        in_part[:, width:] = squares
        send_rows(2 * l, in_part, in_send, in_recv, l)
        loads["in_y%d" % l].wait()
        y_slot = layers + 1 + l
        y_sem = 2 * layers + 2 + l
        o_part[y_slot] = jnp.dot(h, in_y[l], preferred_element_type=F32)
        send_rows(y_sem, o_part.at[y_slot], o_send, o_recv, y_slot)
        both = reduced(2 * l, in_part, in_recv, l)
        scale = mean_scale(both[:, width:])
        driven = (both[:, :width] * scale).astype(BF16).astype(F32)
        if l == 0:
            for name in (
                "conv_w", "conv_b", "conv_s", "lru", "gx_b", "ga_b", "decay", "gx_w", "ga_w"
            ):
                loads[name].wait()
        taps = [conv_s[l, j].astype(F32) for j in range(conv_s.shape[1])]
        taps += [driven[s * batch:(s + 1) * batch] for s in range(steps)]
        count = conv_w.shape[1]
        filtered = conv_b[l:l + 1, :]
        for j in range(count):
            filtered = filtered + conv_w[l, j:j + 1, :] * stack_rows(taps[j:j + steps])
        for j in range(count - 1):
            conv_out[l, j] = taps[steps + j].astype(BF16)
        half = filtered.astype(BF16)
        blocks, size = gx_w.shape[1], gx_w.shape[2]
        gates = []
        for weight, bias in ((gx_w, gx_b), (ga_w, ga_b)):
            mixed = jnp.concatenate(
                [
                    jnp.dot(
                        half[:, k * size:(k + 1) * size], weight[l, k], preferred_element_type=F32
                    )
                    for k in range(blocks)
                ],
                axis=1,
            )
            gates.append(jax.nn.sigmoid(mixed + bias[l:l + 1, :]))
        log_decay = -8.0 * gates[1] * softplus(decay[l:l + 1, :])
        keep = jnp.exp(log_decay)
        add = jnp.sqrt(1.0 - jnp.exp(2.0 * log_decay)) * (gates[0] * filtered)
        index = jnp.full((1, LANES), scale_ref[l], jnp.int32).astype(F32)[:, :1]
        state_scale = jnp.exp2((index - 4.0) * 0.5)
        state = lru[l].astype(F32) * state_scale
        states = []
        for s in range(steps):
            state = keep[s * batch:(s + 1) * batch] * state + add[s * batch:(s + 1) * batch]
            states.append(state)
        lru_out[l] = (state / state_scale).astype(BF16)
        branch = reduced(y_sem, o_part.at[y_slot], o_recv, y_slot) * scale
        gating = jax.nn.gelu(branch, approximate=True)
        mixed = (stack_rows(states) * gating).astype(BF16)
        spreaded = spread(2 * l + 1, mixed)
        loads["rec_out%d" % l].wait()
        o_part[l] = jnp.dot(spreaded, rec_out[l], preferred_element_type=F32)
        send_rows(2 * l + 1, o_part.at[l], o_send, o_recv, l)
        stream = stream + reduced(2 * l + 1, o_part.at[l], o_recv, l)

    raw = spread(2 * layers, stream.astype(BF16))
    loads["attn_gain"].wait()
    h, squares = normed(raw, attn_gain[:, pl.ds(my_block, depth)])
    loads["q_w"].wait()
    loads["kv_w"].wait()
    q_part[:, :width] = jnp.dot(h, q_w[...], preferred_element_type=F32)
    q_part[:, width:width + kv_cols] = jnp.dot(h, kv_w[...], preferred_element_type=F32)
    q_part[:, width + kv_cols:] = squares
    send_rows(2 * layers, q_part, q_send, q_recv, 0)
    both = reduced(2 * layers, q_part, q_recv, 0)
    scale = mean_scale(both[:, width + kv_cols:])
    local = (both[:, :width + kv_cols] * scale).astype(BF16)
    for s in range(steps):
        kv_out[s] = local[s * batch:(s + 1) * batch, width:]
    head_send[...] = local
    for k in range(1, nm):
        pltpu.make_async_remote_copy(
            src_ref=head_send, dst_ref=head_recv.at[me_m],
            send_sem=head_ss.at[0], recv_sem=head_rs.at[0],
            device_id=(me_d, lax.rem(me_m + k, nm)), device_id_type=MESH,
        ).start()
    head_recv[me_m] = local
    window = slots * nm
    row_ids = lax.broadcasted_iota(jnp.int32, (rows, 1), 0)
    row_seq = lax.rem(row_ids, batch)
    row_step = row_ids // batch
    position = jnp.zeros((rows, 1), jnp.int32)
    for b in range(batch):
        position = jnp.where(row_seq == b, pos_ref[b], position)
    column = lax.broadcasted_iota(jnp.int32, (rows, batch * slots), 1)
    slot_id = me_m * slots + lax.rem(column, slots)
    back = lax.rem(position - 1 - slot_id + window, window)
    held = position - 1 - back
    valid = (
        (held >= 0) & (held >= position + row_step - window + 1) & (column // slots == row_seq)
    )
    new_column = lax.broadcasted_iota(jnp.int32, (rows, rows), 1)
    new_valid = (
        (lax.rem(new_column, batch) == row_seq) & (new_column // batch <= row_step) & (me_m == 0)
    )
    loads["keys"].wait()
    loads["values"].wait()
    got = head_recv.at[pl.ds(0, nm - 1)]
    pltpu.make_async_copy(got, got, head_rs.at[0]).wait()
    group = width // head
    heads = nm * group
    query = jnp.concatenate(
        [
            head_recv[m, :, g * head:(g + 1) * head].astype(F32)
            for m in range(nm)
            for g in range(group)
        ],
        axis=0,
    ).astype(BF16)
    fresh = jnp.concatenate([head_recv[m, :, width:] for m in range(nm)], axis=1)
    factor = head ** (-0.5)
    dims_t = (((1,), (1,)), ((), ()))
    cache_keys = keys[...].reshape(batch * slots, head)
    cache_values = values[...].reshape(batch * slots, head)
    scores = lax.dot_general(query, cache_keys, dims_t, preferred_element_type=F32) * factor
    scores = scores.reshape(heads, rows, batch * slots)
    new_scores = lax.dot_general(query, fresh[:, :head], dims_t, preferred_element_type=F32)
    new_scores = (new_scores * factor).reshape(heads, rows, rows)
    scores = jnp.where(valid[None], scores, -1e30)
    new_scores = jnp.where(new_valid[None], new_scores, -1e30)
    top = jnp.maximum(
        jnp.max(scores, axis=-1, keepdims=True), jnp.max(new_scores, axis=-1, keepdims=True)
    )
    weights = jnp.where(valid[None], jnp.exp(scores - top), 0.0)
    new_weights = jnp.where(new_valid[None], jnp.exp(new_scores - top), 0.0)
    weight_sum = jnp.sum(weights, axis=-1, keepdims=True) + jnp.sum(
        new_weights, axis=-1, keepdims=True
    )
    summed = jnp.dot(
        weights.reshape(heads * rows, batch * slots).astype(BF16), cache_values,
        preferred_element_type=F32,
    ) + jnp.dot(
        new_weights.reshape(heads * rows, rows).astype(BF16), fresh[:, head:],
        preferred_element_type=F32,
    )
    top = top.reshape(heads * rows, 1)
    weight_sum = weight_sum.reshape(heads * rows, 1)
    span = group * rows
    lane = lax.broadcasted_iota(jnp.int32, (heads * rows, LANES), 1)
    stats = jnp.where(lane < LANES // 2, top, weight_sum)
    sum_send[...] = summed.astype(BF16).reshape(nm, span, head)
    stat_send[...] = stats.reshape(nm, span, LANES)
    for k in range(1, nm):
        target = lax.rem(me_m + k, nm)
        pltpu.make_async_remote_copy(
            src_ref=sum_send.at[target], dst_ref=sum_recv.at[k - 1],
            send_sem=head_ss.at[1], recv_sem=head_rs.at[1],
            device_id=(me_d, target), device_id_type=MESH,
        ).start()
        pltpu.make_async_remote_copy(
            src_ref=stat_send.at[target], dst_ref=stat_recv.at[k - 1],
            send_sem=head_ss.at[2], recv_sem=head_rs.at[2],
            device_id=(me_d, target), device_id_type=MESH,
        ).start()
    pltpu.make_async_copy(sum_recv, sum_recv, head_rs.at[1]).wait()
    pltpu.make_async_copy(stat_recv, stat_recv, head_rs.at[2]).wait()
    parts = [(sum_send[me_m], stat_send[me_m])]
    parts += [(sum_recv[k], stat_recv[k]) for k in range(nm - 1)]
    tops = [stat[:, :1] for _, stat in parts]
    best = functools.reduce(jnp.maximum, tops)
    fades = [jnp.exp(t - best) for t in tops]
    whole = sum(f * stat[:, LANES // 2:LANES // 2 + 1] for f, (_, stat) in zip(fades, parts))
    mixed = sum(f * part.astype(F32) for f, (part, _) in zip(fades, parts)) / whole
    attended = jnp.concatenate(
        [mixed[g * rows:(g + 1) * rows] for g in range(group)], axis=1
    ).astype(BF16)
    spreaded = spread(2 * layers + 1, attended)
    loads["out_w"].wait()
    o_part[layers] = jnp.dot(spreaded, out_w[...], preferred_element_type=F32)
    send_rows(2 * layers + 1, o_part.at[layers], o_send, o_recv, layers)
    stream = stream + reduced(2 * layers + 1, o_part.at[layers], o_recv, layers)
    for s in range(steps):
        hidden_out[s] = stream[s * batch:(s + 1) * batch].astype(BF16)

    for phase in range(2 * layers + 2):
        @pl.when(is_mine)
        def _(phase=phase):
            part = spread_recv.at[phase, pl.ds(0, nd - 1)]
            pltpu.make_async_copy(part, part, spread_ss.at[phase]).wait()

        @pl.when(jnp.logical_not(is_mine))
        def _(phase=phase):
            part = spread_recv.at[phase]
            pltpu.make_async_copy(part, part, spread_ss.at[phase]).wait()

    for l in range(layers):
        for sem_slot, ref in ((2 * l, in_send), (2 * l + 1, o_send)):
            pltpu.make_async_copy(ref.at[l], ref.at[l], part_ss.at[sem_slot]).wait()
        got = o_send.at[layers + 1 + l]
        pltpu.make_async_copy(got, got, part_ss.at[2 * layers + 2 + l]).wait()
    pltpu.make_async_copy(q_send.at[0], q_send.at[0], part_ss.at[2 * layers]).wait()
    pltpu.make_async_copy(o_send.at[layers], o_send.at[layers], part_ss.at[2 * layers + 1]).wait()
    got = head_recv.at[pl.ds(0, nm - 1)]
    pltpu.make_async_copy(got, got, head_ss.at[0]).wait()
    pltpu.make_async_copy(sum_recv, sum_recv, head_ss.at[1]).wait()
    pltpu.make_async_copy(stat_recv, stat_recv, head_ss.at[2]).wait()


def put_out(*refs):
    copies = [
        pltpu.make_async_copy(refs[i], refs[4 + i], refs[8].at[i]) for i in range(4)
    ]
    for copy in copies:
        copy.start()
    for copy in copies:
        copy.wait()


def body(nd, nm, *args):
    (
        hidden_in, rec_gain, in_x, in_y, conv_w, conv_b, gx_w, gx_b, ga_w, ga_b, decay,
        rec_out, lru, conv_s, scale_index, attn_gain, q_w, kv_w, out_w, keys, values, positions,
    ) = args
    steps, batch, width = hidden_in.shape
    layers, depth = in_x.shape[:2]
    kv_cols = kv_w.shape[1]
    slots, head = keys.shape[1:]
    rows = steps * batch
    per = nd // nm
    group = width // head
    span = group * rows
    dims = (layers, steps, batch, width, depth, kv_cols, slots, head)
    attn_gain = attn_gain.reshape(1, -1)
    args = (
        hidden_in, rec_gain, in_x, in_y, conv_w, conv_b, gx_w, gx_b, ga_w, ga_b, decay,
        rec_out, lru, conv_s, scale_index, attn_gain, q_w, kv_w, out_w, keys, values, positions,
    )
    in_smem = (14, 21)
    in_cols = width + LANES
    q_cols = width + kv_cols + LANES
    phases = 2 * layers + 2
    held = [
        pltpu.VMEM(a.shape, a.dtype) for i, a in enumerate(args) if i not in in_smem
    ]
    any_spec = pl.BlockSpec(memory_space=pl.ANY)
    smem = pl.BlockSpec(memory_space=pltpu.SMEM)
    vmem = pl.BlockSpec(memory_space=pltpu.VMEM)
    shapes = (hidden_in.shape, lru.shape, conv_s.shape, (steps, batch, kv_cols))
    results = pl.pallas_call(
        functools.partial(kernel, nd, nm, dims),
        out_shape=tuple(pltpu.VMEM(shape, BF16) for shape in shapes),
        in_specs=[smem if i in in_smem else any_spec for i in range(len(args))],
        out_specs=(vmem,) * 4,
        scratch_shapes=held + [
            pltpu.VMEM((phases, per, rows, depth), BF16),
            pltpu.VMEM((phases, nd, rows, depth), BF16),
            pltpu.VMEM((nd * rows, in_cols), F32),
            pltpu.VMEM((layers, nd - 1, rows, in_cols), BF16),
            pltpu.VMEM((layers, nd - 1, rows, in_cols), BF16),
            pltpu.VMEM((2 * layers + 1, nd * rows, width), F32),
            pltpu.VMEM((2 * layers + 1, nd - 1, rows, width), BF16),
            pltpu.VMEM((2 * layers + 1, nd - 1, rows, width), BF16),
            pltpu.VMEM((nd * rows, q_cols), F32),
            pltpu.VMEM((1, nd - 1, rows, q_cols), BF16),
            pltpu.VMEM((1, nd - 1, rows, q_cols), BF16),
            pltpu.VMEM((rows, width + kv_cols), BF16),
            pltpu.VMEM((nm, rows, width + kv_cols), BF16),
            pltpu.VMEM((nm, span, head), BF16),
            pltpu.VMEM((nm - 1, span, head), BF16),
            pltpu.VMEM((nm, span, LANES), F32),
            pltpu.VMEM((nm - 1, span, LANES), F32),
            pltpu.SemaphoreType.DMA((23,)),
            pltpu.SemaphoreType.DMA((phases,)),
            pltpu.SemaphoreType.DMA((phases,)),
            pltpu.SemaphoreType.DMA((phases + layers,)),
            pltpu.SemaphoreType.DMA((phases + layers,)),
            pltpu.SemaphoreType.DMA((3,)),
            pltpu.SemaphoreType.DMA((3,)),
            pltpu.SemaphoreType.DMA((phases,)),
        ],
        compiler_params=pltpu.CompilerParams(
            collective_id=0, has_side_effects=True, vmem_limit_bytes=56 * 1024 * 1024
        ),
    )(*args)
    return pl.pallas_call(
        put_out,
        out_shape=tuple(jax.ShapeDtypeStruct(shape, BF16) for shape in shapes),
        in_specs=[vmem] * 4,
        out_specs=(any_spec,) * 4,
        scratch_shapes=[pltpu.SemaphoreType.DMA((4,))],
        compiler_params=pltpu.CompilerParams(vmem_limit_bytes=1024 * 1024),
    )(*results)


def solution(mesh):
    placed = (
        P(None, "dp", "mp"),
        P(),
        P(None, "dp", "mp"),
        P(None, "dp", "mp"),
        P(None, None, "mp"),
        P(None, "mp"),
        P(None, "mp", None, None),
        P(None, "mp"),
        P(None, "mp", None, None),
        P(None, "mp"),
        P(None, "mp"),
        P(None, "dp", "mp"),
        P(None, "dp", "mp"),
        P(None, None, "dp", "mp"),
        P(),
        P(),
        P("dp", "mp"),
        P("dp", "mp"),
        P("dp", "mp"),
        P("dp", "mp", None),
        P("dp", "mp", None),
        P("dp"),
    )
    return jax.shard_map(
        functools.partial(body, mesh.shape["dp"], mesh.shape["mp"]),
        mesh=mesh,
        in_specs=placed,
        out_specs=(
            P(None, "dp", "mp"),
            P(None, "dp", "mp"),
            P(None, None, "dp", "mp"),
            P(None, "dp", "mp"),
        ),
        check_vma=False,
    )
```
